32 devices in a mesh: neg: 8 (over y, x, core), qry: 4 (over z).
Axes of the slice: x: 2, y: 2, z: 4, core: 2. Of those that a mesh axis runs over, the one named last changes fastest.
Arguments:
- items_table: bfloat16 [65536, 512], P('neg'), may hold values from -6 to 6
- fetch_rows: int32 [256, 1280], P(('neg', 'qry')), may hold values from 0 to 8191, as said below
- neighbour_slots: int32 [16384, 40], P(('neg', 'qry')), may hold values from 0 to 10239, as said below
- neighbour_count: int32 [16384], P(('neg', 'qry')), may hold values from 20 to 40
- self_slot: int32 [16384], P(('neg', 'qry')), may hold values from 0 to 10239
- negative_count: int32 [16384], P('neg'), may hold values from 1 to 999
- message_weight: bfloat16 [512, 512], replicated, may hold values from -0.25 to 0.25
- message_bias: float32 [512], replicated, may hold values from -3 to 3
- self_weight: bfloat16 [512, 512], replicated, may hold values from -0.25 to 0.25
- neighbour_weight: bfloat16 [512, 512], replicated, may hold values from -0.25 to 0.25
- output_bias: float32 [512], replicated, may hold values from -3 to 3
- queries: bfloat16 [4096, 512], P('qry'), may hold values from -8 to 8
Outputs:
- negative_embed: bfloat16 [16384, 512], P(('neg', 'qry'))
- query_lse: float32 [4096], P('qry')
The draws below stay inside these ranges and needn't reach their ends.
Inputs may be any that keep to these rules, and one draw needn't show every extreme that they name: Within one row of fetch_rows (one device's list for one partition) no item appears twice. `neighbour_slots`: every one of a device's 8 * 1280 fetched rows is named by at least one live neighbour of that device's negatives.
All inputs are finite; a program needn't handle non-finite values.
Results may differ from the reference program's by a relative error of at most 0.0055.
Values may be sent and summed in bfloat16 or wider, within the bound.
A program may use at most 128 MiB of HBM per device.

```python
import math
import jax
import jax.numpy as jnp
from jax import lax

D = 512
K = 40
ITEM_DEV = 8192
NEG_DEV = 512
CAP = 1280
NEG = 16384
QRY = 4096
ITEMS = 65536
N_NEG = 8
N_QRY = 4


def draw_queries(key, part):
    values = jnp.clip(jax.random.normal(key, (QRY, D), jnp.float32), -5.5, 5.5)
    return values.astype(jnp.bfloat16)


def draw_fetch_rows(key, part):
    row_keys = jax.random.split(jax.random.fold_in(key, 7), N_NEG * N_QRY * N_NEG)

    def one_row(row_key):
        return jax.random.permutation(row_key, ITEM_DEV)[:CAP].astype(jnp.int32)
    return jax.vmap(one_row)(row_keys).astype(jnp.int32)


def neighbour_draw(key):
    count_key = jax.random.fold_in(key, 11)
    counts = jax.random.randint(count_key, (NEG,), K // 2, K + 1, dtype=jnp.int32)
    slot_total = N_NEG * CAP
    device_keys = jax.random.split(jax.random.fold_in(key, 13), N_NEG * N_QRY)
    count_blocks = counts.reshape(N_NEG * N_QRY, NEG_DEV)

    def one_device(device_key, count_block):
        order_key = jax.random.fold_in(device_key, 1)
        filler_key = jax.random.fold_in(device_key, 2)
        live_mask = jnp.arange(K, dtype=jnp.int32)[None, :] < count_block[:, None]
        priority = jax.random.randint(order_key, (NEG_DEV * K,), 0, 1 << 20, dtype=jnp.int32)
        priority = priority + jnp.where(live_mask.reshape(-1), 0, 1 << 21).astype(jnp.int32)
        order = jnp.argsort(priority, stable=True).astype(jnp.int32)
        ranked = jnp.argsort(order, stable=True).astype(jnp.int32)
        filler = jax.random.randint(filler_key, (NEG_DEV * K,), 0, slot_total, dtype=jnp.int32)
        slots = jnp.where(ranked < slot_total, ranked, filler)
        return slots.reshape(NEG_DEV, K).astype(jnp.int32)
    slots = jax.vmap(one_device)(device_keys, count_blocks).reshape(NEG, K)
    return (counts, slots)


def draw_neighbour_count(key, part):
    return neighbour_draw(key)[0].astype(jnp.int32)


def draw_neighbour_slots(key, part):
    return neighbour_draw(key)[1].astype(jnp.int32)


def place_ends(drawn, stream_key, smallest, largest):
    longest = drawn.shape.index(max(drawn.shape))
    spots = []
    for shift in (0, 1):
        where = [jax.random.randint(jax.random.fold_in(stream_key, axis), (), 0, length) for axis, length in enumerate(drawn.shape)]
        where[longest] = (where[longest] + shift) % drawn.shape[longest]
        spots.append(tuple(where))
    return drawn.at[spots[0]].set(smallest).at[spots[1]].set(largest)


def shard_levels(own_key, shape, cuts, least, high):
    factor_of = 1.0
    for dim, parts in cuts:
        draws = jax.random.uniform(jax.random.fold_in(jax.random.fold_in(own_key, 6), dim), (parts,), jnp.float32, least / len(cuts), high / len(cuts))
        factor_of = factor_of * jnp.repeat(jnp.exp(draws), shape[dim] // parts).reshape((-1,) + (1,) * (len(shape) - 1 - dim))
    return factor_of


def gaussian(key, shape, deviation, limit, pieces=(), kind=jnp.bfloat16):
    factor_of = shard_levels(key, shape, pieces, -0.22, 0.18) if pieces else 1.0
    values = jax.random.normal(key, shape, jnp.float32) * deviation * factor_of
    return jnp.minimum(jnp.maximum(values, -limit), limit).astype(kind)


def setup_inputs(seed: int = 0) -> dict:
    seeds = jax.random.split(jax.random.key(seed), 13)
    items_table = gaussian(seeds[0], (ITEMS, D), 1.0, 6.0, ((0, 8),))
    fetch_rows = draw_fetch_rows(jax.random.fold_in(seeds[12], 71), 0)
    neighbour_slots = draw_neighbour_slots(jax.random.fold_in(seeds[12], 71), 0)
    neighbour_count = draw_neighbour_count(jax.random.fold_in(seeds[12], 71), 0)
    self_slot = place_ends(jax.random.randint(seeds[4], (NEG,), 0, N_NEG * CAP), jax.random.fold_in(seeds[4], 1), 0, (N_NEG * CAP) - 1).astype(jnp.int32)
    negative_count = place_ends(jax.random.randint(seeds[5], (NEG,), 1, 1000), jax.random.fold_in(seeds[5], 1), 1, 999).astype(jnp.int32)
    message_weight = gaussian(seeds[6], (D, D), D ** -0.5, 0.25)
    message_bias = gaussian(seeds[7], (D,), 0.5, 3.0, (), jnp.float32)
    self_weight = gaussian(seeds[8], (D, D), D ** -0.5, 0.25)
    neighbour_weight = gaussian(seeds[9], (D, D), D ** -0.5, 0.25)
    output_bias = gaussian(seeds[10], (D,), 0.5, 3.0, (), jnp.float32)
    queries = draw_queries(jax.random.fold_in(seeds[12], 71), 0)
    return {"items_table": items_table, "fetch_rows": fetch_rows, "neighbour_slots": neighbour_slots, "neighbour_count": neighbour_count, "self_slot": self_slot, "negative_count": negative_count, "message_weight": message_weight, "message_bias": message_bias, "self_weight": self_weight, "neighbour_weight": neighbour_weight, "output_bias": output_bias, "queries": queries}


def embed_device(items_table, fetch_block, slot_block, count_block, self_block, message_weight, message_bias, self_weight, neighbour_weight, output_bias):
    owners = jnp.arange(N_NEG, dtype=jnp.int32)[:, None] * ITEM_DEV
    global_rows = (fetch_block.astype(jnp.int32) + owners).reshape(-1)
    fetched = items_table[global_rows]
    message = jax.nn.relu(jnp.dot(fetched, message_weight, preferred_element_type=jnp.float32) + message_bias).astype(jnp.bfloat16)
    gathered = message[slot_block].astype(jnp.float32)
    live_mask = jnp.arange(K, dtype=jnp.int32)[None, :] < count_block[:, None]
    summed = lax.optimization_barrier(jnp.sum(jnp.where(live_mask[:, :, None], gathered, jnp.float32(0.0)), axis=1))
    neighbour_mean = (summed / count_block.astype(jnp.float32)[:, None]).astype(jnp.bfloat16)
    self_rows = fetched[self_block]
    hidden = jnp.dot(self_rows, self_weight, preferred_element_type=jnp.float32)
    hidden = hidden + jnp.dot(neighbour_mean, neighbour_weight, preferred_element_type=jnp.float32) + output_bias
    hidden = jax.nn.relu(hidden)
    scale_inv = lax.rsqrt(lax.optimization_barrier(jnp.mean(hidden * hidden, axis=-1, keepdims=True)) + 0.25)
    return (hidden * scale_inv).astype(jnp.bfloat16)

def reference(items_table, fetch_rows, neighbour_slots, neighbour_count, self_slot, negative_count, message_weight, message_bias, self_weight, neighbour_weight, output_bias, queries):
    devices_all = N_NEG * N_QRY
    fetch_all = fetch_rows.reshape(devices_all, N_NEG, -1)
    slots_all = neighbour_slots.reshape(devices_all, -1, K)
    counts_all = neighbour_count.reshape(devices_all, -1)
    selves_all = self_slot.reshape(devices_all, -1)

    def one_device(inputs):
        return embed_device(items_table, inputs[0], inputs[1], inputs[2], inputs[3], message_weight, message_bias, self_weight, neighbour_weight, output_bias)
    embedded = lax.map(one_device, (fetch_all, slots_all, counts_all, selves_all))
    negative_embed = embedded.reshape(-1, D)
    log_count = jnp.log(negative_count.astype(jnp.float32))
    query_blocks = queries.reshape(N_QRY, -1, D)

    def one_block(query_block):
        scores = 0.25 * jnp.dot(query_block, negative_embed.T, preferred_element_type=jnp.float32) - log_count[None, :]
        peak = lax.optimization_barrier(jnp.max(scores, axis=1))
        totals = lax.optimization_barrier(jnp.sum(jnp.exp(scores - peak[:, None]), axis=1))
        return peak + jnp.log(totals) - math.log(NEG)
    query_lse = lax.map(one_block, query_blocks).reshape(-1)
    return (negative_embed, query_lse)
```

```python
import functools
import math

import jax
import jax.numpy as jnp
from jax import lax
from jax.experimental import pallas as pl
from jax.experimental.pallas import tpu as pltpu
from jax.sharding import PartitionSpec as P


LANES = 128
ROWS = 128
DEAD = 32767
NT = (((1,), (1,)), ((), ()))
MESH = pl.DeviceIdType.MESH
WHOLE = pl.BlockSpec(memory_space=pltpu.VMEM)


def flip(index, mask):
    out = index
    bit = 1
    while bit <= mask:
        if mask & bit:
            out = out + bit * (1 - 2 * ((index // bit) % 2))
        bit *= 2
    return out


def greet(devices):
    barrier = pltpu.get_barrier_semaphore()
    for device in devices:
        pl.semaphore_signal(barrier, inc=1, device_id=device, device_id_type=MESH)
    pl.semaphore_wait(barrier, len(devices))


def sort_pairs(count):
    full = 1
    while full < count:
        full *= 2
    pairs = []
    p = 1
    while p < full:
        k = p
        while k >= 1:
            for j in range(k % p, full - k, 2 * k):
                for i in range(min(k, full - j - k)):
                    if (i + j) // (2 * p) == (i + j + k) // (2 * p):
                        if i + j + k < count:
                            pairs.append((i + j, i + j + k))
            k //= 2
        p *= 2
    return pairs


def exchange_kernel(
    n, lists_ref, fetch_ref, wm_ref, ws_ref, wn_ref,
    lists_out, want_out, wmt_ref, wst_ref, wnt_ref, send_sem, recv_sem,
):
    neg, qry = lax.axis_index("neg"), lax.axis_index("qry")
    greet([(flip(neg, d), qry) for d in range(1, n)])
    copies = []
    for j in range(n - 1):
        d = n - 1 - j
        peer = (flip(neg, d), qry)
        for i, (source, target) in enumerate(
            ((lists_ref, lists_out.at[j]), (fetch_ref.at[flip(neg, d)], want_out.at[j]))
        ):
            copy = pltpu.make_async_remote_copy(
                src_ref=source, dst_ref=target,
                send_sem=send_sem.at[i, j], recv_sem=recv_sem.at[i, j],
                device_id=peer, device_id_type=MESH,
            )
            copy.start()
            copies.append(copy)
    lists_out[n - 1] = lists_ref[...]
    want_out[n - 1] = fetch_ref[neg]
    wmt_ref[...] = wm_ref[...].T
    wst_ref[...] = ws_ref[...].T
    wnt_ref[...] = wn_ref[...].T
    for copy in copies:
        copy.wait()


def exchange(lists, fetch, weights):
    n, height, _ = fetch.shape
    return pl.pallas_call(
        functools.partial(exchange_kernel, n),
        out_shape=[
            jax.ShapeDtypeStruct((n,) + lists.shape, jnp.int32),
            jax.ShapeDtypeStruct(fetch.shape, jnp.int32),
        ]
        + [jax.ShapeDtypeStruct(w.shape[::-1], w.dtype) for w in weights],
        in_specs=[WHOLE] * 5,
        out_specs=[WHOLE] * 5,
        scratch_shapes=[pltpu.SemaphoreType.DMA((2, n)), pltpu.SemaphoreType.DMA((2, n))],
        compiler_params=pltpu.CompilerParams(collective_id=0, has_side_effects=True),
    )(lists, fetch, *weights)


def pick_kernel(
    index_ref, base_ref, table_ref, slots_ref,
    out_ref, counts_ref, scale_ref, wide_ref, picked_ref, order_ref, times_ref,
):
    block = pl.program_id(0)
    rows, width = table_ref.shape
    cap = out_ref.shape[1]
    pieces = width // LANES

    @pl.when(block == 0)
    def _():
        @pl.loop(0, rows // ROWS)
        def _(t):
            span = pl.ds(pl.multiple_of(t * ROWS, ROWS), ROWS)
            for c in range(pieces):
                wide_ref[pl.ds(t * ROWS * pieces + c, ROWS, stride=pieces), :] = table_ref[
                    span, c * LANES : (c + 1) * LANES
                ].astype(jnp.float32)

    unroll = 32

    @pl.loop(0, cap // unroll)
    def _(i):
        first = block * cap + i * unroll
        start = pl.multiple_of(i * (unroll * pieces), unroll * pieces)
        places = [pl.multiple_of(index_ref[first + u], pieces) for u in range(unroll)]
        for u in range(unroll):
            picked_ref[pl.ds(start + u * pieces, pieces), :] = wide_ref[
                pl.ds(places[u], pieces), :
            ]

    @pl.loop(0, cap // ROWS)
    def _(t):
        span = pl.ds(pl.multiple_of(t * ROWS, ROWS), ROWS)
        for c in range(pieces):
            out_ref[0, span, c * LANES : (c + 1) * LANES] = picked_ref[
                pl.ds(t * ROWS * pieces + c, ROWS, stride=pieces), :
            ].astype(jnp.bfloat16)

    negatives = counts_ref.shape[2]
    groups, neighbours = negatives // LANES, times_ref.shape[1]
    half = neighbours // 2
    packed = 16
    chunk = 320 if cap % 320 == 0 else ROWS
    big = jnp.int32(32767)
    base = base_ref[0]
    places = []
    live = jnp.zeros((groups, LANES), jnp.int32)
    mine = jnp.zeros((groups, LANES), jnp.int32)
    for k in range(neighbours):
        word = slots_ref[0, (k % half) * groups : (k % half + 1) * groups, :]
        slot = word & DEAD if k < half else word >> 16
        local = slot - base
        inside = (local >= 0) & (local < cap)
        live = live + jnp.where(slot < DEAD, 1, 0)
        mine = mine + jnp.where(inside, 1, 0)
        places.append(jnp.where(inside, local, big))
    for a, b in sort_pairs(neighbours):
        low, high = jnp.minimum(places[a], places[b]), jnp.maximum(places[a], places[b])
        places[a], places[b] = low, high
    run = jnp.ones((groups, LANES), jnp.float32)
    for k in range(neighbours):
        if k:
            run = jnp.where(places[k] == places[k - 1], run + 1.0, 1.0)
        for g in range(groups):
            tile = (packed, LANES)
            order_ref[g, k] = jnp.broadcast_to(places[k][g : g + 1], tile).astype(jnp.int16)
            times_ref[g, k] = jnp.broadcast_to(run[g : g + 1], tile).astype(jnp.bfloat16)
    scale_ref[0] = 1.0 / live.astype(jnp.float32)
    iota = lax.broadcasted_iota(jnp.int32, (packed, LANES), 0)
    tiles = chunk // packed
    unroll = 4
    for g in range(groups):
        lanes = pl.ds(g * LANES, LANES)
        steps = (jnp.max(mine[g : g + 1]) + unroll - 1) // unroll

        @pl.loop(0, cap // chunk)
        def _(c):
            first = c * chunk
            here = [(iota + (first + packed * i)).astype(jnp.int16) for i in range(tiles)]

            def step(i, totals):
                for u in range(unroll):
                    k = unroll * i + u
                    slot, times = order_ref[g, k], times_ref[g, k]
                    totals = tuple(
                        jnp.where(here[j] == slot, times, totals[j]) for j in range(tiles)
                    )
                return totals

            zero = jnp.zeros((packed, LANES), jnp.bfloat16)
            totals = lax.fori_loop(0, steps, step, (zero,) * tiles)
            for j in range(tiles):
                span = pl.ds(pl.multiple_of(first + packed * j, packed), packed)
                counts_ref[0, span, lanes] = totals[j]


def pick(index, base, table, lists, shape):
    rows, width = table.shape
    n = lists.shape[0]
    cap = index.shape[0] // n
    negatives, neighbours = shape
    groups = negatives // LANES
    pieces = width // LANES
    return pl.pallas_call(
        pick_kernel,
        grid=(n,),
        out_shape=[
            jax.ShapeDtypeStruct((n, cap, width), jnp.bfloat16),
            jax.ShapeDtypeStruct((n, cap, negatives), jnp.bfloat16),
            jax.ShapeDtypeStruct((n, groups, LANES), jnp.float32),
        ],
        in_specs=[
            pl.BlockSpec(memory_space=pltpu.SMEM),
            pl.BlockSpec(memory_space=pltpu.SMEM),
            WHOLE,
            pl.BlockSpec((1,) + lists.shape[1:], lambda b: (b, 0, 0)),
        ],
        out_specs=[
            pl.BlockSpec((1, cap, width), lambda b: (b, 0, 0)),
            pl.BlockSpec((1, cap, negatives), lambda b: (b, 0, 0)),
            pl.BlockSpec((1, groups, LANES), lambda b: (b, 0, 0)),
        ],
        scratch_shapes=[
            pltpu.VMEM((rows * pieces, LANES), jnp.float32),
            pltpu.VMEM((cap * pieces, LANES), jnp.float32),
            pltpu.VMEM((groups, neighbours, 16, LANES), jnp.int16),
            pltpu.VMEM((groups, neighbours, 16, LANES), jnp.bfloat16),
        ],
        compiler_params=pltpu.CompilerParams(vmem_limit_bytes=50 << 20),
    )(index, base, table, lists)


def part_kernel(
    n, rows_ref, counts_ref, scale_ref, lists_ref, wm_ref, mb_ref, ws_ref, wn_ref, bias_ref,
    embed_ref, near_send, near_recv, far_send, far_recv, hot_ref, keep_ref,
    near_ss, near_rs, far_ss, far_rs,
):
    neg, qry = lax.axis_index("neg"), lax.axis_index("qry")
    step = pl.program_id(0)
    cap, negatives = counts_ref.shape[1:]
    groups = negatives // LANES
    packed = 16
    partner = (flip(neg, 1), qry)

    def near_copy(i):
        return pltpu.make_async_remote_copy(
            src_ref=near_send.at[i], dst_ref=near_recv.at[i],
            send_sem=near_ss.at[i], recv_sem=near_rs.at[i],
            device_id=partner, device_id_type=MESH,
        )

    def far_copy(i):
        return pltpu.make_async_remote_copy(
            src_ref=far_send.at[i], dst_ref=far_recv.at[i],
            send_sem=far_ss.at[i], recv_sem=far_rs.at[i],
            device_id=(flip(neg, n - 2 - 2 * i), qry), device_id_type=MESH,
        )

    @pl.when(step == 0)
    def _():
        greet([partner] + [(flip(neg, d), qry) for d in range(2, n, 2)])

    base = neg * cap
    own = lists_ref[0] - base
    own = jnp.where((own >= 0) & (own < cap), own, 32767)
    iota = lax.broadcasted_iota(jnp.int32, (packed, LANES), 0)
    one = jnp.ones((packed, LANES), jnp.bfloat16)
    zero = jnp.zeros((packed, LANES), jnp.bfloat16)
    for g in range(groups):
        tile = jnp.broadcast_to(own[g : g + 1], (packed, LANES)).astype(jnp.int16)
        for t in range(cap // packed):
            here = (iota + packed * t).astype(jnp.int16)
            hot_ref[t * packed : (t + 1) * packed, g * LANES : (g + 1) * LANES] = jnp.where(
                here == tile, one, zero
            )

    rows = rows_ref[0]
    message = jax.nn.relu(
        lax.dot_general(wm_ref[...], rows, NT, preferred_element_type=jnp.float32) + mb_ref[...]
    ).astype(jnp.bfloat16)
    summed = jnp.dot(message, counts_ref[0], preferred_element_type=jnp.float32)
    scale = jnp.concatenate([scale_ref[0, g : g + 1, :] for g in range(groups)], axis=1)
    mean = (summed * scale).astype(jnp.bfloat16)
    own_part = lax.dot_general(ws_ref[...], rows, NT, preferred_element_type=jnp.float32).astype(
        jnp.bfloat16
    )
    part = jnp.dot(own_part, hot_ref[...], preferred_element_type=jnp.float32)
    part = part + jnp.dot(wn_ref[...], mean, preferred_element_type=jnp.float32)
    keep_ref[...] = part

    for j in range(n):
        i = j // 2

        @pl.when(step == j)
        def _():
            if j % 2 == 0:
                near_send[i] = keep_ref[...].astype(jnp.bfloat16)
                near_copy(i).start()
            else:
                near_copy(i).wait_recv()
                if j < n - 1:
                    far_send[i] = (keep_ref[...] + near_recv[i].astype(jnp.float32)).astype(
                        jnp.bfloat16
                    )
                    far_copy(i).start()
                else:
                    hidden = keep_ref[...] + near_recv[i].astype(jnp.float32) + bias_ref[...]
                    for c in range(n // 2 - 1):
                        far_copy(c).wait_recv()
                        hidden = hidden + far_recv[c].astype(jnp.float32)
                    hidden = jax.nn.relu(hidden)
                    scale = lax.rsqrt(jnp.mean(hidden * hidden, axis=0, keepdims=True) + 0.25)
                    embed_ref[...] = (hidden * scale).T.astype(jnp.bfloat16)
                    for c in range(n // 2):
                        near_copy(c).wait_send()
                    for c in range(n // 2 - 1):
                        far_copy(c).wait_send()


def embed(rows, counts, scale, selves, wm, mb, ws, wn, bias):
    n, cap, width = rows.shape
    negatives = counts.shape[2]
    groups = negatives // LANES
    square = (width, negatives)
    return pl.pallas_call(
        functools.partial(part_kernel, n),
        grid=(n,),
        out_shape=jax.ShapeDtypeStruct((negatives, width), jnp.bfloat16),
        in_specs=[
            pl.BlockSpec((1, cap, width), lambda b: (b, 0, 0)),
            pl.BlockSpec((1, cap, negatives), lambda b: (b, 0, 0)),
            pl.BlockSpec((1, groups, LANES), lambda b: (b, 0, 0)),
            pl.BlockSpec((1, groups, LANES), lambda b: (b, 0, 0)),
            WHOLE, WHOLE, WHOLE, WHOLE, WHOLE,
        ],
        out_specs=WHOLE,
        scratch_shapes=[
            pltpu.VMEM((n // 2,) + square, jnp.bfloat16),
            pltpu.VMEM((n // 2,) + square, jnp.bfloat16),
            pltpu.VMEM((n // 2 - 1,) + square, jnp.bfloat16),
            pltpu.VMEM((n // 2 - 1,) + square, jnp.bfloat16),
            pltpu.VMEM((cap, negatives), jnp.bfloat16),
            pltpu.VMEM(square, jnp.float32),
            pltpu.SemaphoreType.DMA((n // 2,)),
            pltpu.SemaphoreType.DMA((n // 2,)),
            pltpu.SemaphoreType.DMA((n // 2 - 1,)),
            pltpu.SemaphoreType.DMA((n // 2 - 1,)),
        ],
        compiler_params=pltpu.CompilerParams(
            collective_id=1, has_side_effects=True, vmem_limit_bytes=56 << 20
        ),
    )(rows, counts, scale, selves, wm, mb, ws, wn, bias)


def score_kernel(n, blocks, *refs):
    query_refs = refs[:blocks]
    embed_ref, count_ref, out_ref, pair_ref, near_ref, whole_ref, far_ref = refs[blocks : blocks + 7]
    near_ss, near_rs, far_ss, far_rs = refs[blocks + 7 :]
    neg, qry = lax.axis_index("neg"), lax.axis_index("qry")
    greet(
        [(neg, flip(qry, d)) for d in range(1, blocks)]
        + [(flip(neg, d), qry) for d in range(1, n)]
    )
    log_count = jnp.log(count_ref[...].astype(jnp.float32))
    rows = query_refs[0].shape[0]
    tile = 512
    copies = []
    for b in list(range(1, blocks)) + [0]:
        target = near_ref.at[0] if b == 0 else pair_ref.at[b]

        @pl.loop(0, rows // tile)
        def _(t):
            span = pl.ds(pl.multiple_of(t * tile, tile), tile)
            scores = (
                0.25
                * lax.dot_general(
                    embed_ref[...], query_refs[b][span, :], NT, preferred_element_type=jnp.float32
                )
                - log_count
            )
            peak = jnp.max(scores, axis=0, keepdims=True)
            target[0:1, span] = peak
            target[1:2, span] = jnp.sum(jnp.exp(scores - peak), axis=0, keepdims=True)

        if b:
            copy = pltpu.make_async_remote_copy(
                src_ref=pair_ref.at[b], dst_ref=near_ref.at[b],
                send_sem=near_ss.at[b], recv_sem=near_rs.at[b],
                device_id=(neg, flip(qry, b)), device_id_type=MESH,
            )
            copy.start()
            copies.append(copy)
    for copy in copies:
        copy.wait()

    def merge(ref, count):
        peaks = [ref[c, 0:1, :] for c in range(count)]
        top = functools.reduce(jnp.maximum, peaks)
        total = functools.reduce(
            jnp.add, [ref[c, 1:2, :] * jnp.exp(peaks[c] - top) for c in range(count)]
        )
        return top, total

    top, total = merge(near_ref, blocks)
    whole_ref[0:1, :] = top
    whole_ref[1:2, :] = total
    far_ref[0, 0:1, :] = top
    far_ref[0, 1:2, :] = total
    copies = []
    for d in range(1, n):
        copy = pltpu.make_async_remote_copy(
            src_ref=whole_ref, dst_ref=far_ref.at[d],
            send_sem=far_ss.at[d], recv_sem=far_rs.at[d],
            device_id=(flip(neg, d), qry), device_id_type=MESH,
        )
        copy.start()
        copies.append(copy)
    for copy in copies:
        copy.wait()
    top, total = merge(far_ref, n)
    negatives = embed_ref.shape[0] * n * blocks
    out_ref[...] = top + jnp.log(total) - math.log(negatives)


def score(queries, negative_embed, count, n):
    blocks = len(queries)
    rows = queries[0].shape[0]
    negatives, width = negative_embed.shape
    return pl.pallas_call(
        functools.partial(score_kernel, n, blocks),
        out_shape=jax.ShapeDtypeStruct((1, rows), jnp.float32),
        in_specs=[WHOLE] * (blocks + 2),
        out_specs=WHOLE,
        scratch_shapes=[
            pltpu.VMEM((blocks, 2, rows), jnp.float32),
            pltpu.VMEM((blocks, 2, rows), jnp.float32),
            pltpu.VMEM((2, rows), jnp.float32),
            pltpu.VMEM((n, 2, rows), jnp.float32),
            pltpu.SemaphoreType.DMA((blocks,)),
            pltpu.SemaphoreType.DMA((blocks,)),
            pltpu.SemaphoreType.DMA((n,)),
            pltpu.SemaphoreType.DMA((n,)),
        ],
        compiler_params=pltpu.CompilerParams(collective_id=2, has_side_effects=True),
    )(*queries, negative_embed, count)


def swap(value, axis, offset):
    size = lax.axis_size(axis)
    if offset == 0:
        return value
    return lax.ppermute(value, axis, [(i, i ^ offset) for i in range(size)])


def per_device(
    items_table,
    fetch_rows,
    neighbour_slots,
    neighbour_count,
    self_slot,
    negative_count,
    message_weight,
    message_bias,
    self_weight,
    neighbour_weight,
    output_bias,
    queries,
):
    n_neg, n_qry = lax.axis_size("neg"), lax.axis_size("qry")
    own_neg, own_qry = lax.axis_index("neg"), lax.axis_index("qry")
    cap = fetch_rows.shape[1]
    pieces = items_table.shape[1] // LANES
    negatives, neighbours = neighbour_slots.shape
    groups = negatives // LANES

    assert n_neg * cap < DEAD and neighbours % 4 == 0
    query_blocks = [queries]
    for d in range(1, n_qry):
        query_blocks.append(swap(queries, "qry", d))

    live = jnp.arange(neighbours, dtype=jnp.int32)[None, :] < neighbour_count[:, None]
    slots = jnp.where(live, neighbour_slots, DEAD).T
    half = neighbours // 2
    words = slots[:half] | (slots[half:] << 16)
    lists = jnp.concatenate([words.reshape(-1, LANES), self_slot.reshape(-1, LANES)])
    fetch = (fetch_rows * pieces).reshape(n_neg, cap // LANES, LANES)
    lists, wanted, wm, ws, wn = exchange(
        lists, fetch, (message_weight, self_weight, neighbour_weight)
    )
    base = (own_neg * cap).astype(jnp.int32).reshape(1)
    rows, counts, scale = pick(
        wanted.reshape(-1), base, items_table, lists, (negatives, neighbours)
    )
    negative_embed = embed(
        rows, counts, scale, lists[:, half * groups :, :],
        wm, message_bias[:, None], ws, wn, output_bias[:, None],
    )
    count = lax.dynamic_slice_in_dim(negative_count, own_qry * negatives, negatives)
    query_lse = score(query_blocks, negative_embed, count[:, None], n_neg)
    return (negative_embed, query_lse.reshape(-1))


def solution(mesh):
    in_specs = (
        P("neg", None),
        P(("neg", "qry"), None),
        P(("neg", "qry"), None),
        P(("neg", "qry")),
        P(("neg", "qry")),
        P("neg"),
        P(),
        P(),
        P(),
        P(),
        P(),
        P("qry", None),
    )
    out_specs = (P(("neg", "qry"), None), P("qry"))
    return jax.shard_map(
        per_device, mesh=mesh, in_specs=in_specs, out_specs=out_specs, check_vma=False
    )
```

```python
import functools
import math

import jax
import jax.numpy as jnp
from jax import lax
from jax.experimental import pallas as pl
from jax.experimental.pallas import tpu as pltpu
from jax.sharding import PartitionSpec as P


LANES = 128
ROWS = 128
DEAD = 32767
NT = (((1,), (1,)), ((), ()))
MESH = pl.DeviceIdType.MESH
WHOLE = pl.BlockSpec(memory_space=pltpu.VMEM)


def flip(index, mask):
    out = index
    bit = 1
    while bit <= mask:
        if mask & bit:
            out = out + bit * (1 - 2 * ((index // bit) % 2))
        bit *= 2
    return out


def greet(devices):
    barrier = pltpu.get_barrier_semaphore()
    for device in devices:
        pl.semaphore_signal(barrier, inc=1, device_id=device, device_id_type=MESH)
    pl.semaphore_wait(barrier, len(devices))


def sort_pairs(count):
    full = 1
    while full < count:
        full *= 2
    pairs = []
    p = 1
    while p < full:
        k = p
        while k >= 1:
            for j in range(k % p, full - k, 2 * k):
                for i in range(min(k, full - j - k)):
                    if (i + j) // (2 * p) == (i + j + k) // (2 * p):
                        if i + j + k < count:
                            pairs.append((i + j, i + j + k))
            k //= 2
        p *= 2
    return pairs


def exchange_kernel(
    n, pieces, slots_ref, self_ref, fetch_ref, wm_ref, ws_ref, wn_ref,
    lists_out, want_out, self_out, wmt_ref, wst_ref, wnt_ref, mine_ref, send_sem, recv_sem,
):
    neg, qry = lax.axis_index("neg"), lax.axis_index("qry")
    groups = self_ref.shape[0]
    neighbours = slots_ref.shape[0] // groups
    half = neighbours // 2
    slots = [slots_ref[k * groups : (k + 1) * groups, :] for k in range(neighbours)]
    for a, b in sort_pairs(neighbours):
        slots[a], slots[b] = jnp.minimum(slots[a], slots[b]), jnp.maximum(slots[a], slots[b])
    for k in range(half):
        mine_ref[k * groups : (k + 1) * groups, :] = slots[k] | (slots[k + half] << 16)
    mine_ref[half * groups :, :] = self_ref[...]
    lists_out[n - 1] = mine_ref[...]
    want_out[n - 1] = fetch_ref[neg]
    greet([(flip(neg, d), qry) for d in range(1, n)])
    copies = []
    for j in range(n - 1):
        d = n - 1 - j
        peer = (flip(neg, d), qry)
        for i, (source, target) in enumerate(
            ((mine_ref, lists_out.at[j]), (fetch_ref.at[flip(neg, d)], want_out.at[j]))
        ):
            copy = pltpu.make_async_remote_copy(
                src_ref=source, dst_ref=target,
                send_sem=send_sem.at[i, j], recv_sem=recv_sem.at[i, j],
                device_id=peer, device_id_type=MESH,
            )
            copy.start()
            copies.append(copy)
    wmt_ref[...] = wm_ref[...].T
    wst_ref[...] = ws_ref[...].T
    wnt_ref[...] = wn_ref[...].T
    for copy in copies:
        copy.wait()
    cap = fetch_ref.shape[1] * fetch_ref.shape[2]
    for j in range(n):
        local = lists_out[j, half * groups :, :] - neg * cap
        self_out[j] = jnp.where((local >= 0) & (local < cap), local, cap) * pieces


def exchange(slots, selves, fetch, weights, pieces):
    n = fetch.shape[0]
    groups = selves.shape[0]
    height = slots.shape[0] // 2 + groups
    return pl.pallas_call(
        functools.partial(exchange_kernel, n, pieces),
        out_shape=[
            jax.ShapeDtypeStruct((n, height, LANES), jnp.int32),
            jax.ShapeDtypeStruct(fetch.shape, jnp.int32),
            jax.ShapeDtypeStruct((n,) + selves.shape, jnp.int32),
        ]
        + [jax.ShapeDtypeStruct(w.shape[::-1], w.dtype) for w in weights],
        in_specs=[WHOLE] * 6,
        out_specs=[WHOLE] * 6,
        scratch_shapes=[
            pltpu.VMEM((height, LANES), jnp.int32),
            pltpu.SemaphoreType.DMA((2, n)),
            pltpu.SemaphoreType.DMA((2, n)),
        ],
        compiler_params=pltpu.CompilerParams(collective_id=0, has_side_effects=True),
    )(slots, selves, fetch, *weights)


def count_kernel(
    n, base_ref, want_ref, self_ref, table_ref, lists_ref,
    rows_ref, counts_ref, scale_ref,
    word_ref, bit_ref, once_ref, run_ref, low_ref, high_ref,
    near_ref, wide_ref, picked_ref, selves_ref, load_sem,
):
    step = pl.program_id(0)
    rows, width = table_ref.shape
    pieces = width // LANES
    share = rows // n
    cap, negatives = counts_ref.shape[1:]
    groups = negatives // LANES
    neighbours = word_ref.shape[0]
    half = neighbours // 2
    sublanes, packed = 8, 16
    stacks = low_ref.shape[0] // sublanes

    def load(t):
        span = pl.ds(t * share, share)
        return pltpu.make_async_copy(table_ref.at[span], near_ref.at[span], load_sem.at[t])

    @pl.when(step == 0)
    def _():
        for t in range(n):
            load(t).start()
        picked_ref[cap * pieces :, :] = jnp.zeros((8, LANES), jnp.float32)

    base = base_ref[0]
    live = jnp.zeros((groups, LANES), jnp.int32)
    longest = jnp.zeros((groups, LANES), jnp.int32)
    last = run = None
    for k in range(neighbours):
        word = lists_ref[0, (k % half) * groups : (k % half + 1) * groups, :]
        slot = word & DEAD if k < half else word >> 16
        local = slot - base
        inside = (local >= 0) & (local < cap)
        live = live + jnp.where(slot < DEAD, 1, 0)
        run = jnp.where(slot == last, run + 1, 1) if k else jnp.ones_like(slot)
        last = slot
        longest = jnp.maximum(longest, jnp.where(inside, run, 0))
        word_ref[k] = local >> 5
        bit = jnp.where(inside, jnp.left_shift(1, local & 31), 0)
        bit_ref[k] = bit
        once_ref[k] = jnp.where(run == 1, bit, 0)
        run_ref[k] = run
    scale_ref[0] = 1.0 / live.astype(jnp.float32)
    iota = lax.broadcasted_iota(jnp.int32, (sublanes, LANES), 0)
    deep = lax.broadcasted_iota(jnp.int32, (packed, LANES), 0)
    mask = jnp.left_shift(1, deep).astype(jnp.int16)
    one = jnp.ones((packed, LANES), jnp.bfloat16)
    zero = jnp.zeros((packed, LANES), jnp.bfloat16)

    def plane(g, level):
        found = [jnp.zeros((sublanes, LANES), jnp.int32) for _ in range(stacks)]
        for k in range(neighbours):
            if level is None:
                bit = once_ref[k, g : g + 1, :]
            else:
                bit = bit_ref[k, g : g + 1, :]
                bit = jnp.where(run_ref[k, g : g + 1, :] == level, bit, 0)
            bit = jnp.broadcast_to(bit, (sublanes, LANES))
            place = jnp.broadcast_to(word_ref[k, g : g + 1, :], (sublanes, LANES))
            for i in range(stacks):
                found[i] = found[i] | jnp.where(iota + sublanes * i == place, bit, 0)
        for i in range(stacks):
            span = slice(i * sublanes, (i + 1) * sublanes)
            low_ref[span, :] = found[i]
            high_ref[span, :] = found[i] >> 16

    def tiles(g, add):
        for t in range(cap // packed):
            source = high_ref if t % 2 else low_ref
            bits = jnp.broadcast_to(source[t // 2 : t // 2 + 1, :], (packed, LANES))
            count = jnp.where((bits.astype(jnp.int16) & mask) != 0, one, zero)
            spot = (0, slice(t * packed, (t + 1) * packed), slice(g * LANES, (g + 1) * LANES))
            counts_ref[spot] = counts_ref[spot] + count if add else count

    @pl.when(step == 0)
    def _():
        for t in range(n):
            load(t).wait()

            @pl.loop(0, share // ROWS)
            def _(i):
                first = (t * (share // ROWS) + i) * ROWS
                span = pl.ds(pl.multiple_of(first, ROWS), ROWS)
                for c in range(pieces):
                    wide_ref[pl.ds(first * pieces + c, ROWS, stride=pieces), :] = near_ref[
                        span, c * LANES : (c + 1) * LANES
                    ].astype(jnp.float32)

    def gather(first, count):
        for u in range(first, first + count):
            place = pl.multiple_of(want_ref[step, u // LANES, u % LANES], pieces)
            picked_ref[u * pieces : (u + 1) * pieces, :] = wide_ref[pl.ds(place, pieces), :]
        for c in range(pieces):
            rows_ref[0, first : first + count, c * LANES : (c + 1) * LANES] = picked_ref[
                pl.ds(first * pieces + c, count, stride=pieces), :
            ].astype(jnp.bfloat16)

    part = cap // groups
    for g in range(groups):
        plane(g, None)
        tiles(g, False)
        gather(g * part, part)
        most = jnp.max(longest[g : g + 1])

        @pl.loop(2, most + 1)
        def _(level):
            plane(g, level)
            tiles(g, True)

    for g in range(groups):
        for u in range(LANES):
            place = pl.multiple_of(self_ref[step, g, u], pieces)
            selves_ref[(g * LANES + u) * pieces : (g * LANES + u + 1) * pieces, :] = picked_ref[
                pl.ds(place, pieces), :
            ]
    for c in range(pieces):
        rows_ref[0, cap:, c * LANES : (c + 1) * LANES] = selves_ref[
            pl.ds(c, negatives, stride=pieces), :
        ].astype(jnp.bfloat16)


def count(base, want, selves, table, lists, shape):
    n = lists.shape[0]
    rows, width = table.shape
    pieces = width // LANES
    cap = want.shape[1] * want.shape[2]
    negatives, neighbours = shape
    groups = negatives // LANES
    stacks = -(-cap // 256)
    small = pltpu.VMEM((neighbours, groups, LANES), jnp.int32)
    scalars = pl.BlockSpec(memory_space=pltpu.SMEM)

    def block(*shape):
        return pl.BlockSpec((1,) + shape, lambda b: (b, 0, 0))

    return pl.pallas_call(
        functools.partial(count_kernel, n),
        grid=(n,),
        out_shape=[
            jax.ShapeDtypeStruct((n, cap + negatives, width), jnp.bfloat16),
            jax.ShapeDtypeStruct((n, cap, negatives), jnp.bfloat16),
            jax.ShapeDtypeStruct((n, groups, LANES), jnp.float32),
        ],
        in_specs=[
            scalars,
            scalars,
            scalars,
            pl.BlockSpec(memory_space=pl.ANY),
            block(*lists.shape[1:]),
        ],
        out_specs=[block(cap + negatives, width), block(cap, negatives), block(groups, LANES)],
        scratch_shapes=[
            small, small, small, small,
            pltpu.VMEM((stacks * 8, LANES), jnp.int32),
            pltpu.VMEM((stacks * 8, LANES), jnp.int32),
            pltpu.VMEM((rows, width), jnp.bfloat16),
            pltpu.VMEM((rows * pieces, LANES), jnp.float32),
            pltpu.VMEM((cap * pieces + 8, LANES), jnp.float32),
            pltpu.VMEM((negatives * pieces, LANES), jnp.float32),
            pltpu.SemaphoreType.DMA((n,)),
        ],
        compiler_params=pltpu.CompilerParams(vmem_limit_bytes=60 << 20),
    )(base, want, selves, table, lists)


def part_kernel(
    n, rows_ref, counts_ref, scale_ref,
    wm_ref, mb_ref, ws_ref, wn_ref, bias_ref,
    embed_ref, near_send, near_recv, far_send, far_recv, keep_ref, mb_col, bias_col,
    near_ss, near_rs, far_ss, far_rs,
):
    neg, qry = lax.axis_index("neg"), lax.axis_index("qry")
    step = pl.program_id(0)
    cap, negatives = counts_ref.shape[1:]
    groups = negatives // LANES
    partner = (flip(neg, 1), qry)

    def near_copy(i):
        return pltpu.make_async_remote_copy(
            src_ref=near_send.at[i], dst_ref=near_recv.at[i],
            send_sem=near_ss.at[i], recv_sem=near_rs.at[i],
            device_id=partner, device_id_type=MESH,
        )

    def far_copy(i):
        return pltpu.make_async_remote_copy(
            src_ref=far_send.at[i], dst_ref=far_recv.at[i],
            send_sem=far_ss.at[i], recv_sem=far_rs.at[i],
            device_id=(flip(neg, n - 2 - 2 * i), qry), device_id_type=MESH,
        )

    @pl.when(step == 0)
    def _():
        tall = (LANES, mb_ref.shape[1])
        mb_col[...] = jnp.broadcast_to(mb_ref[...], tall).T
        bias_col[...] = jnp.broadcast_to(bias_ref[...], tall).T
        greet([partner] + [(flip(neg, d), qry) for d in range(2, n, 2)])

    message = jax.nn.relu(
        lax.dot_general(
            wm_ref[...], rows_ref[0, :cap, :], NT, preferred_element_type=jnp.float32
        )
        + mb_col[:, 0:1]
    ).astype(jnp.bfloat16)
    summed = jnp.dot(message, counts_ref[0], preferred_element_type=jnp.float32)
    scale = jnp.concatenate([scale_ref[0, g : g + 1, :] for g in range(groups)], axis=1)
    mean = (summed * scale).astype(jnp.bfloat16)
    part = lax.dot_general(
        ws_ref[...], rows_ref[0, cap:, :], NT, preferred_element_type=jnp.float32
    )
    part = part + jnp.dot(wn_ref[...], mean, preferred_element_type=jnp.float32)
    keep_ref[...] = part

    for j in range(n):
        i = j // 2

        @pl.when(step == j)
        def _():
            if j % 2 == 0:
                near_send[i] = keep_ref[...].astype(jnp.bfloat16)
                near_copy(i).start()
            else:
                near_copy(i).wait_recv()
                if j < n - 1:
                    far_send[i] = (keep_ref[...] + near_recv[i].astype(jnp.float32)).astype(
                        jnp.bfloat16
                    )
                    far_copy(i).start()
                else:
                    hidden = keep_ref[...] + near_recv[i].astype(jnp.float32) + bias_col[:, 0:1]
                    for c in range(n // 2 - 1):
                        far_copy(c).wait_recv()
                        hidden = hidden + far_recv[c].astype(jnp.float32)
                    hidden = jax.nn.relu(hidden)
                    scale = lax.rsqrt(jnp.mean(hidden * hidden, axis=0, keepdims=True) + 0.25)
                    embed_ref[...] = (hidden * scale).T.astype(jnp.bfloat16)
                    for c in range(n // 2):
                        near_copy(c).wait_send()
                    for c in range(n // 2 - 1):
                        far_copy(c).wait_send()


def embed(rows, counts, scale, wm, mb, ws, wn, bias):
    n, deep, width = rows.shape
    cap, negatives = counts.shape[1:]
    groups = negatives // LANES
    square = (width, negatives)
    return pl.pallas_call(
        functools.partial(part_kernel, n),
        grid=(n,),
        out_shape=jax.ShapeDtypeStruct((negatives, width), jnp.bfloat16),
        in_specs=[
            pl.BlockSpec((1, deep, width), lambda b: (b, 0, 0)),
            pl.BlockSpec((1, cap, negatives), lambda b: (b, 0, 0)),
            pl.BlockSpec((1, groups, LANES), lambda b: (b, 0, 0)),
            WHOLE, WHOLE, WHOLE, WHOLE, WHOLE,
        ],
        out_specs=WHOLE,
        scratch_shapes=[
            pltpu.VMEM((n // 2,) + square, jnp.bfloat16),
            pltpu.VMEM((n // 2,) + square, jnp.bfloat16),
            pltpu.VMEM((n // 2 - 1,) + square, jnp.bfloat16),
            pltpu.VMEM((n // 2 - 1,) + square, jnp.bfloat16),
            pltpu.VMEM(square, jnp.float32),
            pltpu.VMEM((width, LANES), jnp.float32),
            pltpu.VMEM((width, LANES), jnp.float32),
            pltpu.SemaphoreType.DMA((n // 2,)),
            pltpu.SemaphoreType.DMA((n // 2,)),
            pltpu.SemaphoreType.DMA((n // 2 - 1,)),
            pltpu.SemaphoreType.DMA((n // 2 - 1,)),
        ],
        compiler_params=pltpu.CompilerParams(
            collective_id=1, has_side_effects=True, vmem_limit_bytes=60 << 20
        ),
    )(rows, counts, scale, wm, mb, ws, wn, bias)


def score_kernel(n, blocks, *refs):
    own_ref, half_refs = refs[0], refs[1:blocks]
    embed_ref, count_ref, out_ref = refs[blocks : blocks + 3]
    query_ref, pair_ref, near_ref, whole_ref, far_ref = refs[blocks + 3 : blocks + 8]
    load_sem, core_ss, core_rs, near_ss, near_rs, far_ss, far_rs = refs[blocks + 8 :]
    neg, qry = lax.axis_index("neg"), lax.axis_index("qry")
    rows = own_ref.shape[0]
    tile = rows // 2
    side = neg % 2
    loads = [pltpu.make_async_copy(own_ref, query_ref.at[0], load_sem.at[0])]
    for b in range(1, blocks):
        mine = pl.ds(pl.multiple_of(side * tile, tile), tile)
        loads.append(
            pltpu.make_async_copy(half_refs[b - 1], query_ref.at[b, mine], load_sem.at[b])
        )
    for load in loads:
        load.start()
    greet(
        [(flip(neg, d), qry) for d in range(1, n)]
        + [(neg, flip(qry, d)) for d in range(1, blocks)]
    )
    swaps = []
    for b in range(1, blocks):
        copy = pltpu.make_async_remote_copy(
            src_ref=half_refs[b - 1], dst_ref=query_ref.at[b, mine],
            send_sem=core_ss.at[b], recv_sem=core_rs.at[b],
            device_id=(flip(neg, 1), qry), device_id_type=MESH,
        )
        copy.start()
        swaps.append(copy)
    width = embed_ref.shape[0]
    log_count = jnp.log(count_ref[pl.ds(qry, 1), :].astype(jnp.float32))
    log_count = jnp.broadcast_to(log_count, (LANES, width)).T[:, 0:1]

    def tile_of(b, which, target):
        span = pl.ds(pl.multiple_of(which * tile, tile), tile)
        scores = (
            0.25
            * lax.dot_general(
                embed_ref[...], query_ref[b, span, :], NT, preferred_element_type=jnp.float32
            )
            - log_count
        )
        peak = jnp.max(scores, axis=0, keepdims=True)
        target[0:1, span] = peak
        target[1:2, span] = jnp.sum(jnp.exp(scores - peak), axis=0, keepdims=True)

    loads[0].wait()

    @pl.loop(0, 2)
    def _(which):
        tile_of(0, which, near_ref.at[0])

    for load in loads[1:]:
        load.wait()

    @pl.loop(1, blocks)
    def _(b):
        tile_of(b, side, pair_ref.at[b])

    for copy in swaps:
        copy.wait()

    @pl.loop(1, blocks)
    def _(b):
        tile_of(b, 1 - side, pair_ref.at[b])

    copies = []
    for b in range(1, blocks):
        copy = pltpu.make_async_remote_copy(
            src_ref=pair_ref.at[b], dst_ref=near_ref.at[b],
            send_sem=near_ss.at[b], recv_sem=near_rs.at[b],
            device_id=(neg, flip(qry, b)), device_id_type=MESH,
        )
        copy.start()
        copies.append(copy)
    for copy in copies:
        copy.wait()

    def merge(ref, count):
        peaks = [ref[c, 0:1, :] for c in range(count)]
        top = functools.reduce(jnp.maximum, peaks)
        total = functools.reduce(
            jnp.add, [ref[c, 1:2, :] * jnp.exp(peaks[c] - top) for c in range(count)]
        )
        return top, total

    top, total = merge(near_ref, blocks)
    whole_ref[0:1, :] = top
    whole_ref[1:2, :] = total
    far_ref[0, 0:1, :] = top
    far_ref[0, 1:2, :] = total
    copies = []
    for d in range(1, n):
        copy = pltpu.make_async_remote_copy(
            src_ref=whole_ref, dst_ref=far_ref.at[d],
            send_sem=far_ss.at[d], recv_sem=far_rs.at[d],
            device_id=(flip(neg, d), qry), device_id_type=MESH,
        )
        copy.start()
        copies.append(copy)
    for copy in copies:
        copy.wait()
    top, total = merge(far_ref, n)
    negatives = embed_ref.shape[0] * n * blocks
    out_ref[...] = top + jnp.log(total) - math.log(negatives)


def score(queries, halves, negative_embed, count, n):
    blocks = len(halves) + 1
    rows, width = queries.shape
    anywhere = pl.BlockSpec(memory_space=pl.ANY)
    return pl.pallas_call(
        functools.partial(score_kernel, n, blocks),
        out_shape=jax.ShapeDtypeStruct((1, rows), jnp.float32),
        in_specs=[anywhere] * blocks + [WHOLE] * 2,
        out_specs=WHOLE,
        scratch_shapes=[
            pltpu.VMEM((blocks, rows, width), jnp.bfloat16),
            pltpu.VMEM((blocks, 2, rows), jnp.float32),
            pltpu.VMEM((blocks, 2, rows), jnp.float32),
            pltpu.VMEM((2, rows), jnp.float32),
            pltpu.VMEM((n, 2, rows), jnp.float32),
            pltpu.SemaphoreType.DMA((blocks,)),
            pltpu.SemaphoreType.DMA((blocks,)),
            pltpu.SemaphoreType.DMA((blocks,)),
            pltpu.SemaphoreType.DMA((blocks,)),
            pltpu.SemaphoreType.DMA((blocks,)),
            pltpu.SemaphoreType.DMA((n,)),
            pltpu.SemaphoreType.DMA((n,)),
        ],
        compiler_params=pltpu.CompilerParams(
            collective_id=2, has_side_effects=True, vmem_limit_bytes=40 << 20
        ),
    )(queries, *halves, negative_embed, count)


def swap(value, axis, offset):
    size = lax.axis_size(axis)
    if offset == 0:
        return value
    return lax.ppermute(value, axis, [(i, i ^ offset) for i in range(size)])


def per_device(
    items_table,
    fetch_rows,
    neighbour_slots,
    neighbour_count,
    self_slot,
    negative_count,
    message_weight,
    message_bias,
    self_weight,
    neighbour_weight,
    output_bias,
    queries,
):
    n_neg, n_qry = lax.axis_size("neg"), lax.axis_size("qry")
    own_neg = lax.axis_index("neg")
    cap = fetch_rows.shape[1]
    pieces = items_table.shape[1] // LANES
    negatives, neighbours = neighbour_slots.shape
    groups = negatives // LANES

    assert n_neg * cap < DEAD and neighbours % 4 == 0
    part = queries.shape[0] // 2
    half_block = lax.dynamic_slice_in_dim(queries, (own_neg % 2) * part, part)
    halves = [swap(half_block, "qry", d) for d in range(1, n_qry)]

    live = jnp.arange(neighbours, dtype=jnp.int32)[None, :] < neighbour_count[:, None]
    slots = jnp.where(live, neighbour_slots, DEAD).T.reshape(-1, LANES)
    lists, wanted, selves, wm, ws, wn = exchange(
        slots,
        self_slot.reshape(groups, LANES),
        (fetch_rows * pieces).reshape(n_neg, cap // LANES, LANES),
        (message_weight, self_weight, neighbour_weight),
        pieces,
    )
    base = (own_neg * cap).astype(jnp.int32).reshape(1)
    rows, counts, scale = count(
        base, wanted, selves, items_table, lists, (negatives, neighbours)
    )
    negative_embed = embed(
        rows, counts, scale,
        wm, message_bias[None, :], ws, wn, output_bias[None, :],
    )
    drawn = negative_count.reshape(n_qry, negatives)
    query_lse = score(queries, halves, negative_embed, drawn, n_neg)
    return (negative_embed, query_lse.reshape(-1))


def solution(mesh):
    in_specs = (
        P("neg", None),
        P(("neg", "qry"), None),
        P(("neg", "qry"), None),
        P(("neg", "qry")),
        P(("neg", "qry")),
        P("neg"),
        P(),
        P(),
        P(),
        P(),
        P(),
        P("qry", None),
    )
    out_specs = (P(("neg", "qry"), None), P("qry"))
    return jax.shard_map(
        per_device, mesh=mesh, in_specs=in_specs, out_specs=out_specs, check_vma=False
    )
```
